32 devices in a mesh: blk: 4 (over x, core), grp: 8 (over z, y).
Axes of the slice: x: 2, y: 2, z: 4, core: 2. Of those that a mesh axis runs over, the one named last changes fastest.
Arguments:
- text: bfloat16 [32, 512], P(('blk', 'grp')), may hold values from -20 to 20
- keys: bfloat16 [32, 196, 512], P(('blk', 'grp')), may hold values from -400 to 400
- values: bfloat16 [32, 196, 512], P(('blk', 'grp')), may hold values from -5 to 5
- pair_image: int32 [32], replicated, may hold values from 0 to 31, each once
Outputs:
- caption_loss: float32 [32], P(('blk', 'grp'))
- grad_text: float32 [32, 512], P(('blk', 'grp'))
- grad_keys: float32 [32, 196, 512], P(('blk', 'grp'))
- grad_values: float32 [32, 196, 512], P(('blk', 'grp'))
The draws below stay inside these ranges and needn't reach their ends.
All inputs are finite; a program needn't handle non-finite values.
Results may differ from the reference program's by a relative error of at most 0.008.
Values may be sent and summed in bfloat16 or wider, within the bound.
A program may use at most 64 MiB of HBM per device.

```python
import jax
import jax.numpy as jnp
from jax import lax

D = 512
HEADS = 8
PATCHES = 196
IMAGES = 32
CAPTIONS = 32


def shared_text(key):
    base = jax.random.normal(jax.random.fold_in(key, 11), (CAPTIONS, D), jnp.float32)
    base = jnp.clip(base, -4.0, 4.0)
    return base


def draw_text(key, part):
    return shared_text(key).astype(jnp.bfloat16)


def draw_keys(key, part):
    base = jax.random.normal(jax.random.fold_in(key, 13), (IMAGES, PATCHES, D), jnp.float32)
    base = jnp.clip(base, -4.0, 4.0)
    return base.astype(jnp.bfloat16)


def level_of(stream_key, extent, cuts, low, largest):
    def one(dim, blocks):
        steps = jax.random.uniform(jax.random.fold_in(jax.random.fold_in(stream_key, 6), dim), (blocks,), jnp.float32, low / len(cuts), largest / len(cuts))
        return jnp.repeat(jnp.exp(steps), extent[dim] // blocks).reshape((-1,) + (1,) * (len(extent) - dim - 1))

    loudness = one(*cuts[0])
    for cut in cuts[1:]:
        loudness = loudness * one(*cut)
    return loudness


def bell_draw(rng, extent, scale, limit, cuts=(), kind=jnp.bfloat16):
    entries = jax.random.normal(rng, extent, jnp.float32) * scale
    if len(cuts) > 0:
        entries = level_of(rng, extent, cuts, -0.22, 0.18) * entries
    return jnp.clip(entries, min=-limit, max=limit).astype(kind)


def setup_inputs(seed: int = 0) -> dict:
    arg_keys = jax.random.split(jax.random.key(seed), 5)
    text = draw_text(jax.random.fold_in(arg_keys[4], 71), 0)
    keys = draw_keys(jax.random.fold_in(arg_keys[4], 71), 0)
    values = bell_draw(arg_keys[2], (IMAGES, PATCHES, D), 1.0, 5.0, ((0, 32),))
    pair_image = jax.random.permutation(arg_keys[3], IMAGES).astype(jnp.int32)
    return dict(text=text, keys=keys, values=values, pair_image=pair_image)


EPS = 1e-06
LOGIT_SCALE = 10.0
LOGIT_BIAS = -1.0

def image_terms(text, normed, tnorm, pairs, image_id, keys_one, values_one):
    count = text.shape[0]
    width = text.shape[1]
    depth = width // HEADS
    queries = text.astype(jnp.float32).reshape(count, HEADS, depth)
    patch_keys = keys_one.astype(jnp.float32).reshape(-1, HEADS, depth)
    patch_values = values_one.astype(jnp.float32).reshape(-1, HEADS, depth)
    hi = lax.Precision.HIGHEST
    scores = jnp.einsum('chd,phd->chp', queries, patch_keys, precision=hi) * depth ** (-0.5)
    weights = jax.nn.softmax(scores, axis=-1)
    attn = weights.astype(jnp.bfloat16)
    attn_wide = attn.astype(jnp.float32)
    pooled = jnp.einsum('chp,phd->chd', attn_wide, patch_values, precision=hi).reshape(count, width)
    pnorm = lax.rsqrt(lax.optimization_barrier(jnp.mean(pooled * pooled, -1, keepdims=True)) + EPS)
    unit = pooled * pnorm
    cosine = lax.optimization_barrier(jnp.mean(unit * normed, -1))
    logit = LOGIT_SCALE * cosine + LOGIT_BIAS
    label = jnp.where(pairs == image_id, 1.0, -1.0).astype(jnp.float32)
    loss = jax.nn.softplus(-label * logit)
    slope = -label * jax.nn.sigmoid(-label * logit)
    dcos = LOGIT_SCALE / width * slope[:, None]
    dunit = dcos * normed
    dnormed = dcos * unit
    dpool = pnorm * (dunit - unit * lax.optimization_barrier(jnp.mean(dunit * unit, -1, keepdims=True)))
    dout = dpool.astype(jnp.bfloat16).astype(jnp.float32).reshape(count, HEADS, depth)
    dattn = jnp.einsum('chd,phd->chp', dout, patch_values, precision=hi)
    grad_v = jnp.einsum('chp,chd->phd', attn_wide, dout, precision=hi).reshape(-1, width)
    dscore = weights * (dattn - lax.optimization_barrier(jnp.sum(weights * dattn, -1, keepdims=True))) * depth ** (-0.5)
    dscore = dscore.astype(jnp.bfloat16).astype(jnp.float32)
    grad_q = jnp.einsum('chp,phd->chd', dscore, patch_keys, precision=hi).reshape(count, width)
    grad_k = jnp.einsum('chp,chd->phd', dscore, queries, precision=hi).reshape(-1, width)
    grad_x = grad_q + tnorm * (dnormed - normed * lax.optimization_barrier(jnp.mean(dnormed * normed, -1, keepdims=True)))
    return (loss, grad_x, grad_k, grad_v)

def reference(text, keys, values, pair_image):
    count = text.shape[0]
    text_wide = text.astype(jnp.float32)
    tnorm = lax.rsqrt(lax.optimization_barrier(jnp.mean(text_wide * text_wide, -1, keepdims=True)) + EPS)
    normed = text_wide * tnorm
    image_ids = jnp.arange(IMAGES, dtype=jnp.int32)

    def one_image(carry, item):
        keys_one, values_one, image_id = item
        loss, grad_x, grad_k, grad_v = image_terms(text, normed, tnorm, pair_image, image_id, keys_one, values_one)
        return ((carry[0] + loss, carry[1] + grad_x), (grad_k, grad_v))
    start = (jnp.zeros((count,), jnp.float32), jnp.zeros((count, D), jnp.float32))
    (loss_sum, grad_text), (grad_keys, grad_values) = lax.scan(one_image, start, (keys, values, image_ids))
    return (loss_sum / IMAGES, grad_text, grad_keys, grad_values)
```

```python
import functools
import math

import jax
import jax.numpy as jnp
from jax import lax
from jax.experimental import pallas as pl
from jax.experimental.pallas import tpu as pltpu
from jax.sharding import PartitionSpec as P

HEADS = 8
EPS = 1e-06
LOGIT_SCALE = 10.0
LOGIT_BIAS = -1.0
LANES = 128
CHUNK = 32
MESH = pl.DeviceIdType.MESH
LAST = (((1,), (1,)), ((), ()))
FIRST = (((0,), (0,)), ((), ()))


def matmul(a, b, dims=None):
    if dims is None:
        return jnp.dot(a, b, preferred_element_type=jnp.float32)
    return lax.dot_general(a, b, dims, preferred_element_type=jnp.float32)


def kernel(
    groups, members,
    text_hbm, keys_hbm, values_hbm, pair_hbm,
    loss_out, text_out, keys_out, values_out,
    text_own, text_all, keys, values, pairs, part, landed,
    in_sem, pair_sem, gather_send, gather_recv, part_send, part_recv,
):
    n = groups * members
    width = keys.shape[1]
    tiles = width // LANES
    depth = width // HEADS
    me = lax.axis_index("blk") * members + lax.axis_index("grp")

    def device(i):
        return (i // members, lax.rem(i, members))

    text_in = pltpu.make_async_copy(text_hbm, text_own, in_sem.at[0])
    keys_in = pltpu.make_async_copy(keys_hbm.at[0], keys, in_sem.at[1])
    values_in = pltpu.make_async_copy(values_hbm.at[0], values, in_sem.at[2])
    pair_in = pltpu.make_async_copy(pair_hbm, pairs, pair_sem)
    text_in.start()
    barrier = pltpu.get_barrier_semaphore()

    def greet(k, _):
        pl.semaphore_signal(
            barrier, inc=1, device_id=device(lax.rem(me + k, n)), device_id_type=MESH
        )
        return 0

    lax.fori_loop(1, n, greet, 0)
    pair_in.start()
    keys_in.start()
    values_in.start()
    text_in.wait()
    own = text_own[...].astype(jnp.float32)
    for j in range(tiles):
        text_all[me, j : j + 1, :] = own[:, j * LANES : (j + 1) * LANES]
    pl.semaphore_wait(barrier, n - 1)

    def spread(k, _):
        pltpu.make_async_remote_copy(
            src_ref=text_all.at[me],
            dst_ref=text_all.at[me],
            send_sem=gather_send,
            recv_sem=gather_recv,
            device_id=device(lax.rem(me + k, n)),
            device_id_type=MESH,
        ).start()
        return 0

    lax.fori_loop(1, n, spread, 0)
    pair_in.wait()
    keys_in.wait()
    values_in.wait()

    def all_of(ref, sem):
        some = ref.at[pl.ds(0, n - 1)]
        pltpu.make_async_copy(some, some, sem).wait()

    count = min(CHUNK, n)
    chunks = n // count
    low_one = lax.broadcasted_iota(jnp.int32, (count, LANES), 1) < depth
    rows = lax.broadcasted_iota(jnp.int32, (count, 1), 0)

    def halves(x):
        zero = jnp.zeros_like(x)
        return jnp.concatenate(
            [jnp.where(low_one, x, zero), jnp.where(low_one, zero, x)], axis=0
        ).astype(jnp.bfloat16)

    def joined(x):
        return jnp.where(low_one, x[:count], x[count:])

    def total(terms):
        return jnp.sum(functools.reduce(lambda a, b: a + b, terms), axis=1, keepdims=True)

    def mine_of(base):
        def look(i, found):
            return jnp.where(rows == i, pairs[base + i], found)

        found = lax.fori_loop(0, count, look, jnp.zeros((count, 1), jnp.int32))
        return jnp.where(found == me, 1.0, -1.0).astype(jnp.float32)

    def tile(ref, j):
        return ref[:, j * LANES : (j + 1) * LANES]

    def one_chunk(base, label, first):
        text = [text_all[pl.ds(base, count), j, :] for j in range(tiles)]
        tnorm = lax.rsqrt(total([t * t for t in text]) / width + EPS)
        normed = [t * tnorm for t in text]
        queries = [halves(t) for t in text]
        weights, attn, pooled = [], [], []
        for j in range(tiles):
            scores = matmul(queries[j], tile(keys, j), LAST)
            top = jnp.max(scores, axis=1, keepdims=True)
            raised = jnp.exp2((scores - top) * (depth ** (-0.5) * math.log2(math.e)))
            weight = raised * (1.0 / jnp.sum(raised, axis=1, keepdims=True))
            weights.append(weight)
            attn.append(weight.astype(jnp.bfloat16))
            pooled.append(joined(matmul(attn[j], tile(values, j))))
        pnorm = lax.rsqrt(total([p * p for p in pooled]) / width + EPS)
        cosine = pnorm * (total([p * t for p, t in zip(pooled, normed)]) / width)
        unit = [p * pnorm for p in pooled]
        logit = LOGIT_SCALE * cosine + LOGIT_BIAS
        z = -label * logit
        loss = jnp.maximum(z, 0.0) + jnp.log1p(jnp.exp(-jnp.abs(z)))
        dcos = LOGIT_SCALE / width * (-label / (1.0 + jnp.exp(-z)))
        into = pnorm * dcos
        back = tnorm * dcos
        dout, dscore = [], []
        for j in range(tiles):
            dout.append(halves(into * (normed[j] - unit[j] * cosine)))
            dattn = matmul(dout[j], tile(values, j), LAST)
            level = jnp.sum(weights[j] * dattn, axis=1, keepdims=True)
            dscore.append(
                (weights[j] * (dattn - level) * depth ** (-0.5)).astype(jnp.bfloat16)
            )
            grad = joined(matmul(dscore[j], tile(keys, j)))
            part[pl.ds(base, count), j, :] = grad + back * (unit[j] - normed[j] * cosine)
        part[pl.ds(base, count), tiles, :] = jnp.broadcast_to(loss, (count, LANES))

        def deliver(k, _):
            to = base + lax.rem(me + k, count)

            @pl.when(to != me)
            def _():
                pltpu.make_async_remote_copy(
                    src_ref=part.at[to],
                    dst_ref=landed.at[me],
                    send_sem=part_send,
                    recv_sem=part_recv,
                    device_id=device(to),
                    device_id_type=MESH,
                ).start()

            return 0

        lax.fori_loop(0, count, deliver, 0)
        for j in range(tiles):
            lanes = pl.ds(j * LANES, LANES)
            gk = matmul(dscore[j], queries[j], FIRST)
            gv = matmul(attn[j], dout[j], FIRST)
            if first:
                keys_out[0, :, lanes] = gk
                values_out[0, :, lanes] = gv
            else:
                keys_out[0, :, lanes] += gk
                values_out[0, :, lanes] += gv

    if chunks == 1:
        label = mine_of(0)
        all_of(text_all, gather_recv)
        one_chunk(0, label, True)
    else:
        all_of(text_all, gather_recv)
        keys_out[...] = jnp.zeros_like(keys_out)
        values_out[...] = jnp.zeros_like(values_out)

        def body(c, _):
            base = pl.multiple_of(c * count, count)
            one_chunk(base, mine_of(base), False)
            return 0

        lax.fori_loop(0, chunks, body, 0)
    landed[me] = part[me]
    all_of(part, part_recv)
    if chunks == 1:
        got = functools.reduce(lambda a, b: a + b, [landed[i] for i in range(n)])
    else:
        got = lax.fori_loop(
            0, n, lambda i, a: a + landed[i], jnp.zeros(landed.shape[1:], jnp.float32)
        )
    for j in range(tiles):
        text_out[:, j * LANES : (j + 1) * LANES] = got[j : j + 1]
    loss_out[...] = got[tiles : tiles + 1, 0:1] / n
    all_of(text_all, gather_send)
    all_of(part, part_send)


def local(groups, members, text, keys, values, pair_image):
    n = groups * members
    patches, width = keys.shape[1:]
    tiles = width // LANES
    anywhere = pl.BlockSpec(memory_space=pl.ANY)
    vmem = pl.BlockSpec(memory_space=pltpu.VMEM)
    loss, grad_text, grad_keys, grad_values = pl.pallas_call(
        functools.partial(kernel, groups, members),
        out_shape=(
            jax.ShapeDtypeStruct((1, 1), jnp.float32),
            jax.ShapeDtypeStruct(text.shape, jnp.float32),
            jax.ShapeDtypeStruct(keys.shape, jnp.float32),
            jax.ShapeDtypeStruct(values.shape, jnp.float32),
        ),
        in_specs=[anywhere] * 4,
        out_specs=(vmem, vmem, vmem, vmem),
        scratch_shapes=[
            pltpu.VMEM(text.shape, jnp.bfloat16),
            pltpu.VMEM((n, tiles, LANES), jnp.float32),
            pltpu.VMEM((patches, width), jnp.bfloat16),
            pltpu.VMEM((patches, width), jnp.bfloat16),
            pltpu.SMEM((n,), jnp.int32),
            pltpu.VMEM((n, tiles + 1, LANES), jnp.float32),
            pltpu.VMEM((n, tiles + 1, LANES), jnp.float32),
            pltpu.SemaphoreType.DMA((3,)),
            pltpu.SemaphoreType.DMA,
            pltpu.SemaphoreType.DMA,
            pltpu.SemaphoreType.DMA,
            pltpu.SemaphoreType.DMA,
            pltpu.SemaphoreType.DMA,
        ],
        compiler_params=pltpu.CompilerParams(collective_id=0, has_side_effects=True),
        name="pool",
    )(text, keys, values, pair_image)
    return loss.reshape(1), grad_text, grad_keys, grad_values


def solution(mesh):
    groups, members = mesh.shape["blk"], mesh.shape["grp"]
    both = ("blk", "grp")
    placed = (P(both, None), P(both, None, None), P(both, None, None), P())
    return jax.shard_map(
        functools.partial(local, groups, members),
        mesh=mesh,
        in_specs=placed,
        out_specs=(P(both), P(both, None), P(both, None, None), P(both, None, None)),
        check_vma=False,
    )
```

```python
import functools
import math

import jax
import jax.numpy as jnp
from jax import lax
from jax.experimental import pallas as pl
from jax.experimental.pallas import tpu as pltpu
from jax.sharding import PartitionSpec as P

HEADS = 8
EPS = 1e-06
LOGIT_SCALE = 10.0
LOGIT_BIAS = -1.0
LANES = 128
CHUNK = 32
LOGICAL = pl.DeviceIdType.LOGICAL
LAST = (((1,), (1,)), ((), ()))
FIRST = (((0,), (0,)), ((), ()))


def matmul(a, b, dims=None):
    if dims is None:
        return jnp.dot(a, b, preferred_element_type=jnp.float32)
    return lax.dot_general(a, b, dims, preferred_element_type=jnp.float32)


def kernel(
    groups, members,
    text_hbm, keys_hbm, values_hbm, pair_hbm,
    loss_out, text_out, keys_out, values_out,
    text_own, text_all, wide, keys, values, pairs, part, landed,
    in_sem, pair_sem, gather_send, gather_recv, part_send, part_recv,
):
    n = groups * members
    width = keys.shape[1]
    tiles = width // LANES
    depth = width // HEADS
    me = lax.axis_index("blk") * members + lax.axis_index("grp")

    def peer(k):
        other = me + k
        return jnp.where(other >= n, other - n, other)

    def each(low, high, step):
        if high - low <= CHUNK:
            for k in range(low, high):
                step(k)
        else:

            def body(k, _):
                step(k)
                return 0

            lax.fori_loop(low, high, body, 0)

    text_in = pltpu.make_async_copy(text_hbm, text_own, in_sem.at[0])
    keys_in = pltpu.make_async_copy(keys_hbm.at[0], keys, in_sem.at[1])
    values_in = pltpu.make_async_copy(values_hbm.at[0], values, in_sem.at[2])
    pair_in = pltpu.make_async_copy(pair_hbm, pairs, pair_sem)
    text_in.start()
    barrier = pltpu.get_barrier_semaphore()

    def greet(k):
        pl.semaphore_signal(barrier, inc=1, device_id=peer(k), device_id_type=LOGICAL)

    each(1, n, greet)
    pair_in.start()
    keys_in.start()
    values_in.start()
    text_in.wait()
    own = text_own[...].astype(jnp.float32)
    text_all[me] = jnp.concatenate(
        [own[:, j * LANES : (j + 1) * LANES] for j in range(tiles)], axis=0
    ).astype(jnp.bfloat16)
    pl.semaphore_wait(barrier, n - 1)

    def spread(k):
        pltpu.make_async_remote_copy(
            src_ref=text_all.at[me],
            dst_ref=text_all.at[me],
            send_sem=gather_send,
            recv_sem=gather_recv,
            device_id=peer(k),
            device_id_type=LOGICAL,
        ).start()

    each(1, n, spread)
    pair_in.wait()
    keys_in.wait()
    values_in.wait()

    def all_of(ref, sem):
        some = ref.at[pl.ds(0, n - 1)]
        pltpu.make_async_copy(some, some, sem).wait()

    count = min(CHUNK, n)
    chunks = n // count
    low_one = lax.broadcasted_iota(jnp.int32, (count, LANES), 1) < depth
    rows = lax.broadcasted_iota(jnp.int32, (count, 1), 0)

    def halves(x):
        zero = jnp.zeros_like(x)
        return jnp.concatenate(
            [jnp.where(low_one, x, zero), jnp.where(low_one, zero, x)], axis=0
        ).astype(jnp.bfloat16)

    def joined(x):
        return jnp.where(low_one, x[:count], x[count:])

    def total(terms):
        return jnp.sum(functools.reduce(lambda a, b: a + b, terms), axis=1, keepdims=True)

    def mine_of(base):
        found = jnp.zeros((count, 1), jnp.int32)
        for i in range(count):
            found = jnp.where(rows == i, pairs[base + i], found)
        return jnp.where(found == me, 1.0, -1.0).astype(jnp.float32)

    def tile(ref, j):
        return ref[:, j * LANES : (j + 1) * LANES]

    def one_chunk(base, label, first):
        wide[...] = text_all[pl.ds(base, count)].astype(jnp.float32)
        text = [wide[:, j, :] for j in range(tiles)]
        tnorm = lax.rsqrt(total([t * t for t in text]) / width + EPS)
        normed = [t * tnorm for t in text]
        queries = [halves(t) for t in text]
        weights, attn, pooled = [], [], []
        for j in range(tiles):
            scores = matmul(queries[j], tile(keys, j), LAST)
            top = jnp.max(scores, axis=1, keepdims=True)
            raised = jnp.exp2((scores - top) * (depth ** (-0.5) * math.log2(math.e)))
            weight = raised * (1.0 / jnp.sum(raised, axis=1, keepdims=True))
            weights.append(weight)
            attn.append(weight.astype(jnp.bfloat16))
            pooled.append(joined(matmul(attn[j], tile(values, j))))
        pnorm = lax.rsqrt(total([p * p for p in pooled]) / width + EPS)
        cosine = pnorm * (total([p * t for p, t in zip(pooled, normed)]) / width)
        unit = [p * pnorm for p in pooled]
        logit = LOGIT_SCALE * cosine + LOGIT_BIAS
        z = -label * logit
        loss = jnp.maximum(z, 0.0) + jnp.log1p(jnp.exp(-jnp.abs(z)))
        dcos = LOGIT_SCALE / width * (-label / (1.0 + jnp.exp(-z)))
        into = pnorm * dcos
        back = tnorm * dcos
        dout, dscore = [], []
        for j in range(tiles):
            dout.append(halves(into * (normed[j] - unit[j] * cosine)))
            dattn = matmul(dout[j], tile(values, j), LAST)
            level = jnp.sum(weights[j] * dattn, axis=1, keepdims=True)
            dscore.append(
                (weights[j] * (dattn - level) * depth ** (-0.5)).astype(jnp.bfloat16)
            )
            grad = joined(matmul(dscore[j], tile(keys, j)))
            part[pl.ds(base, count), j, :] = grad + back * (unit[j] - normed[j] * cosine)
        part[pl.ds(base, count), tiles, :] = jnp.broadcast_to(loss, (count, LANES))

        def deliver(to):
            pltpu.make_async_remote_copy(
                src_ref=part.at[to],
                dst_ref=landed.at[me],
                send_sem=part_send,
                recv_sem=part_recv,
                device_id=to,
                device_id_type=LOGICAL,
            ).start()

        if first:
            each(1, n, lambda k: deliver(peer(k)))
        else:
            each(0, count, lambda k: pl.when(base + k != me)(lambda: deliver(base + k)))
        for j in range(tiles):
            lanes = pl.ds(j, keys.shape[0], stride=tiles)
            gk = matmul(dscore[j], queries[j], FIRST)
            gv = matmul(attn[j], dout[j], FIRST)
            if first:
                keys_out[lanes, :] = gk
                values_out[lanes, :] = gv
            else:
                keys_out[lanes, :] += gk
                values_out[lanes, :] += gv

    if chunks == 1:
        label = mine_of(0)
        all_of(text_all, gather_recv)
        one_chunk(0, label, True)
    else:
        all_of(text_all, gather_recv)
        keys_out[...] = jnp.zeros_like(keys_out)
        values_out[...] = jnp.zeros_like(values_out)

        def body(c, _):
            base = pl.multiple_of(c * count, count)
            one_chunk(base, mine_of(base), False)
            return 0

        lax.fori_loop(0, chunks, body, 0)
    landed[me] = part[me]
    all_of(part, part_recv)
    if chunks == 1:
        got = functools.reduce(lambda a, b: a + b, [landed[i] for i in range(n)])
    else:
        got = lax.fori_loop(
            0, n, lambda i, a: a + landed[i], jnp.zeros(landed.shape[1:], jnp.float32)
        )
    for j in range(tiles):
        text_out[:, j * LANES : (j + 1) * LANES] = got[j : j + 1]
    loss_out[...] = got[tiles : tiles + 1, 0:1] / n
    all_of(text_all, gather_send)
    all_of(part, part_send)


def local(groups, members, text, keys, values, pair_image):
    n = groups * members
    patches, width = keys.shape[1:]
    tiles = width // LANES
    anywhere = pl.BlockSpec(memory_space=pl.ANY)
    vmem = pl.BlockSpec(memory_space=pltpu.VMEM)
    loss, grad_text, grad_keys, grad_values = pl.pallas_call(
        functools.partial(kernel, groups, members),
        out_shape=(
            pltpu.VMEM((1, 1), jnp.float32),
            pltpu.VMEM(text.shape, jnp.float32),
            pltpu.VMEM((patches * tiles, LANES), jnp.float32),
            pltpu.VMEM((patches * tiles, LANES), jnp.float32),
        ),
        in_specs=[anywhere] * 4,
        out_specs=(vmem, vmem, vmem, vmem),
        scratch_shapes=[
            pltpu.VMEM(text.shape, jnp.bfloat16),
            pltpu.VMEM((n, tiles, LANES), jnp.bfloat16),
            pltpu.VMEM((min(CHUNK, n), tiles, LANES), jnp.float32),
            pltpu.VMEM((patches, width), jnp.bfloat16),
            pltpu.VMEM((patches, width), jnp.bfloat16),
            pltpu.SMEM((n,), jnp.int32),
            pltpu.VMEM((n, tiles + 1, LANES), jnp.float32),
            pltpu.VMEM((n, tiles + 1, LANES), jnp.float32),
            pltpu.SemaphoreType.DMA((3,)),
            pltpu.SemaphoreType.DMA,
            pltpu.SemaphoreType.DMA,
            pltpu.SemaphoreType.DMA,
            pltpu.SemaphoreType.DMA,
            pltpu.SemaphoreType.DMA,
        ],
        compiler_params=pltpu.CompilerParams(collective_id=0, has_side_effects=True),
        name="pool",
    )(text, keys, values, pair_image)
    return (
        loss.reshape(1),
        grad_text,
        grad_keys.reshape(keys.shape),
        grad_values.reshape(values.shape),
    )


def solution(mesh):
    groups, members = mesh.shape["blk"], mesh.shape["grp"]
    both = ("blk", "grp")
    placed = (P(both, None), P(both, None, None), P(both, None, None), P())
    return jax.shard_map(
        functools.partial(local, groups, members),
        mesh=mesh,
        in_specs=placed,
        out_specs=(P(both), P(both, None), P(both, None, None), P(both, None, None)),
        check_vma=False,
    )
```

```python
import functools
import math

import jax
import jax.numpy as jnp
from jax import lax
from jax.experimental import pallas as pl
from jax.experimental.pallas import tpu as pltpu
from jax.sharding import PartitionSpec as P

HEADS = 8
EPS = 1e-06
LOGIT_SCALE = 10.0
LOGIT_BIAS = -1.0
LANES = 128
CHUNK = 32
LOGICAL = pl.DeviceIdType.LOGICAL
LAST = (((1,), (1,)), ((), ()))
FIRST = (((0,), (0,)), ((), ()))


def matmul(a, b, dims=None):
    if dims is None:
        return jnp.dot(a, b, preferred_element_type=jnp.float32)
    return lax.dot_general(a, b, dims, preferred_element_type=jnp.float32)


def kernel(
    groups, members,
    text_hbm, keys_hbm, values_hbm, pair_hbm,
    loss_out, text_out, keys_out, values_out,
    text_own, text_all, wide, keys, values, pairs, part, landed,
    in_sem, pair_sem, gather_send, gather_recv, part_send, part_recv,
):
    n = groups * members
    width = keys.shape[1]
    tiles = width // LANES
    depth = width // HEADS
    me = lax.axis_index("blk") * members + lax.axis_index("grp")

    def peer(k):
        other = me + k
        return jnp.where(other >= n, other - n, other)

    def each(low, high, step):
        if high - low <= CHUNK:
            for k in range(low, high):
                step(k)
        else:

            def body(k, _):
                step(k)
                return 0

            lax.fori_loop(low, high, body, 0)

    text_in = pltpu.make_async_copy(text_hbm, text_own, in_sem.at[0])
    keys_in = pltpu.make_async_copy(keys_hbm.at[0], keys, in_sem.at[1])
    values_in = pltpu.make_async_copy(values_hbm.at[0], values, in_sem.at[2])
    pair_in = pltpu.make_async_copy(pair_hbm, pairs, pair_sem)
    text_in.start()
    barrier = pltpu.get_barrier_semaphore()

    def greet(k):
        pl.semaphore_signal(barrier, inc=1, device_id=peer(k), device_id_type=LOGICAL)

    each(1, n, greet)
    pair_in.start()
    keys_in.start()
    values_in.start()
    text_in.wait()
    own = text_own[...].astype(jnp.float32)
    text_all[me] = jnp.concatenate(
        [own[:, j * LANES : (j + 1) * LANES] for j in range(tiles)], axis=0
    ).astype(jnp.bfloat16)
    pl.semaphore_wait(barrier, n - 1)

    def spread(k):
        pltpu.make_async_remote_copy(
            src_ref=text_all.at[me],
            dst_ref=text_all.at[me],
            send_sem=gather_send,
            recv_sem=gather_recv,
            device_id=peer(k),
            device_id_type=LOGICAL,
        ).start()

    each(1, n, spread)
    pair_in.wait()
    keys_in.wait()
    values_in.wait()

    def all_of(ref, sem):
        some = ref.at[pl.ds(0, n - 1)]
        pltpu.make_async_copy(some, some, sem).wait()

    count = min(CHUNK, n)
    chunks = n // count
    low_one = lax.broadcasted_iota(jnp.int32, (count, LANES), 1) < depth
    rows = lax.broadcasted_iota(jnp.int32, (count, 1), 0)

    def halves(x):
        zero = jnp.zeros_like(x)
        return jnp.concatenate(
            [jnp.where(low_one, x, zero), jnp.where(low_one, zero, x)], axis=0
        ).astype(jnp.bfloat16)

    def joined(x):
        return jnp.where(low_one, x[:count], x[count:])

    def total(terms):
        return jnp.sum(functools.reduce(lambda a, b: a + b, terms), axis=1, keepdims=True)

    def mine_of(base):
        found = jnp.zeros((count, 1), jnp.int32)
        for i in range(count):
            found = jnp.where(rows == i, pairs[base + i], found)
        return jnp.where(found == me, 1.0, -1.0).astype(jnp.float32)

    def tile(ref, j):
        return ref[:, j * LANES : (j + 1) * LANES]

    def one_chunk(base, label, first):
        wide[...] = text_all[pl.ds(base, count)].astype(jnp.float32)
        text = [wide[:, j, :] for j in range(tiles)]
        tnorm = lax.rsqrt(total([t * t for t in text]) / width + EPS)
        normed = [t * tnorm for t in text]
        queries = [halves(t) for t in text]
        weights, attn, pooled = [], [], []
        for j in range(tiles):
            scores = matmul(queries[j], tile(keys, j), LAST)
            top = jnp.max(scores, axis=1, keepdims=True)
            raised = jnp.exp2((scores - top) * (depth ** (-0.5) * math.log2(math.e)))
            weight = raised * (1.0 / jnp.sum(raised, axis=1, keepdims=True))
            weights.append(weight)
            attn.append(weight.astype(jnp.bfloat16))
            pooled.append(joined(matmul(attn[j], tile(values, j))))
        pnorm = lax.rsqrt(total([p * p for p in pooled]) / width + EPS)
        cosine = pnorm * (total([p * t for p, t in zip(pooled, normed)]) / width)
        unit = [p * pnorm for p in pooled]
        logit = LOGIT_SCALE * cosine + LOGIT_BIAS
        z = -label * logit
        loss = jnp.maximum(z, 0.0) + jnp.log1p(jnp.exp(-jnp.abs(z)))
        dcos = LOGIT_SCALE / width * (-label / (1.0 + jnp.exp(-z)))
        into = pnorm * dcos
        back = tnorm * dcos
        dout, dscore = [], []
        for j in range(tiles):
            dout.append(halves(into * (normed[j] - unit[j] * cosine)))
            dattn = matmul(dout[j], tile(values, j), LAST)
            level = jnp.sum(weights[j] * dattn, axis=1, keepdims=True)
            dscore.append(
                (weights[j] * (dattn - level) * depth ** (-0.5)).astype(jnp.bfloat16)
            )
            grad = joined(matmul(dscore[j], tile(keys, j)))
            part[pl.ds(base, count), j, :] = grad + back * (unit[j] - normed[j] * cosine)
        part[pl.ds(base, count), tiles, :] = jnp.broadcast_to(loss, (count, LANES))

        def deliver(to):
            pltpu.make_async_remote_copy(
                src_ref=part.at[to],
                dst_ref=landed.at[me],
                send_sem=part_send,
                recv_sem=part_recv,
                device_id=to,
                device_id_type=LOGICAL,
            ).start()

        if first:
            each(1, n, lambda k: deliver(peer(k)))
        else:
            each(0, count, lambda k: pl.when(base + k != me)(lambda: deliver(base + k)))
        for j in range(tiles):
            lanes = pl.ds(j, keys.shape[0], stride=tiles)
            gk = matmul(dscore[j], queries[j], FIRST)
            gv = matmul(attn[j], dout[j], FIRST)
            if first:
                keys_out[lanes, :] = gk
                values_out[lanes, :] = gv
            else:
                keys_out[lanes, :] += gk
                values_out[lanes, :] += gv

    if chunks == 1:
        label = mine_of(0)
        all_of(text_all, gather_recv)
        one_chunk(0, label, True)
    else:
        all_of(text_all, gather_recv)
        keys_out[...] = jnp.zeros_like(keys_out)
        values_out[...] = jnp.zeros_like(values_out)

        def body(c, _):
            base = pl.multiple_of(c * count, count)
            one_chunk(base, mine_of(base), False)
            return 0

        lax.fori_loop(0, chunks, body, 0)
    landed[me] = part[me]
    all_of(part, part_recv)
    if chunks == 1:
        got = functools.reduce(lambda a, b: a + b, [landed[i] for i in range(n)])
    else:
        got = lax.fori_loop(
            0, n, lambda i, a: a + landed[i], jnp.zeros(landed.shape[1:], jnp.float32)
        )
    for j in range(tiles):
        text_out[:, j * LANES : (j + 1) * LANES] = got[j : j + 1]
    loss_out[...] = got[tiles : tiles + 1, 0:1] / n
    all_of(text_all, gather_send)
    all_of(part, part_send)


def store(*refs):
    sources, targets, sem = refs[:4], refs[4:8], refs[8]
    copies = [
        pltpu.make_async_copy(source, target, sem.at[i])
        for i, (source, target) in enumerate(zip(sources, targets))
    ]
    for copy in copies:
        copy.start()
    for copy in copies:
        copy.wait()


def local(groups, members, text, keys, values, pair_image):
    n = groups * members
    patches, width = keys.shape[1:]
    tiles = width // LANES
    anywhere = pl.BlockSpec(memory_space=pl.ANY)
    vmem = pl.BlockSpec(memory_space=pltpu.VMEM)
    results = pl.pallas_call(
        functools.partial(kernel, groups, members),
        out_shape=(
            pltpu.VMEM((1, 1), jnp.float32),
            pltpu.VMEM(text.shape, jnp.float32),
            pltpu.VMEM((patches * tiles, LANES), jnp.float32),
            pltpu.VMEM((patches * tiles, LANES), jnp.float32),
        ),
        in_specs=[anywhere] * 4,
        out_specs=(vmem, vmem, vmem, vmem),
        scratch_shapes=[
            pltpu.VMEM(text.shape, jnp.bfloat16),
            pltpu.VMEM((n, tiles, LANES), jnp.bfloat16),
            pltpu.VMEM((min(CHUNK, n), tiles, LANES), jnp.float32),
            pltpu.VMEM((patches, width), jnp.bfloat16),
            pltpu.VMEM((patches, width), jnp.bfloat16),
            pltpu.SMEM((n,), jnp.int32),
            pltpu.VMEM((n, tiles + 1, LANES), jnp.float32),
            pltpu.VMEM((n, tiles + 1, LANES), jnp.float32),
            pltpu.SemaphoreType.DMA((3,)),
            pltpu.SemaphoreType.DMA,
            pltpu.SemaphoreType.DMA,
            pltpu.SemaphoreType.DMA,
            pltpu.SemaphoreType.DMA,
            pltpu.SemaphoreType.DMA,
        ],
        compiler_params=pltpu.CompilerParams(collective_id=0, has_side_effects=True),
        name="pool",
    )(text, keys, values, pair_image)
    results = [pltpu.with_memory_space_constraint(r, pltpu.VMEM) for r in results]
    loss, grad_text, grad_keys, grad_values = pl.pallas_call(
        store,
        out_shape=[jax.ShapeDtypeStruct(r.shape, r.dtype) for r in results],
        in_specs=[vmem] * 4,
        out_specs=[anywhere] * 4,
        scratch_shapes=[pltpu.SemaphoreType.DMA((4,))],
        name="store",
    )(*results)
    return (
        loss.reshape(1),
        grad_text,
        grad_keys.reshape(keys.shape),
        grad_values.reshape(values.shape),
    )


def solution(mesh):
    groups, members = mesh.shape["blk"], mesh.shape["grp"]
    both = ("blk", "grp")
    placed = (P(both, None), P(both, None, None), P(both, None, None), P())
    return jax.shard_map(
        functools.partial(local, groups, members),
        mesh=mesh,
        in_specs=placed,
        out_specs=(P(both), P(both, None), P(both, None, None), P(both, None, None)),
        check_vma=False,
    )
```

```python
import functools
import math

import jax
import jax.numpy as jnp
from jax import lax
from jax.experimental import pallas as pl
from jax.experimental.pallas import tpu as pltpu
from jax.sharding import PartitionSpec as P

HEADS = 8
EPS = 1e-06
LOGIT_SCALE = 10.0
LOGIT_BIAS = -1.0
LANES = 128
CHUNK = 32
LOGICAL = pl.DeviceIdType.LOGICAL
LAST = (((1,), (1,)), ((), ()))
FIRST = (((0,), (0,)), ((), ()))


def matmul(a, b, dims=None):
    if dims is None:
        return jnp.dot(a, b, preferred_element_type=jnp.float32)
    return lax.dot_general(a, b, dims, preferred_element_type=jnp.float32)


def kernel(
    groups, members,
    text_hbm, keys_hbm, values_hbm, pair_hbm,
    loss_out, text_out, keys_out, values_out,
    text_own, text_all, wide, keys, values, pairs, part, landed,
    in_sem, pair_sem, gather_send, gather_recv, part_send, part_recv,
):
    n = groups * members
    width = keys.shape[1]
    tiles = width // LANES
    depth = width // HEADS
    me = lax.axis_index("blk") * members + lax.axis_index("grp")

    def peer(k):
        other = me + k
        return jnp.where(other >= n, other - n, other)

    def each(low, high, step):
        if high - low <= CHUNK:
            for k in range(low, high):
                step(k)
        else:

            def body(k, _):
                step(k)
                return 0

            lax.fori_loop(low, high, body, 0)

    text_in = pltpu.make_async_copy(text_hbm, text_own, in_sem.at[0])
    keys_in = pltpu.make_async_copy(keys_hbm.at[0], keys, in_sem.at[1])
    values_in = pltpu.make_async_copy(values_hbm.at[0], values, in_sem.at[2])
    pair_in = pltpu.make_async_copy(pair_hbm, pairs, pair_sem)
    text_in.start()
    barrier = pltpu.get_barrier_semaphore()

    def greet(k):
        pl.semaphore_signal(barrier, inc=1, device_id=peer(k), device_id_type=LOGICAL)

    each(1, n, greet)
    pair_in.start()
    keys_in.start()
    values_in.start()
    text_in.wait()
    own = text_own[...].astype(jnp.float32)
    text_all[me] = jnp.concatenate(
        [own[:, j * LANES : (j + 1) * LANES] for j in range(tiles)], axis=0
    ).astype(jnp.bfloat16)
    pl.semaphore_wait(barrier, n - 1)

    def spread(k):
        pltpu.make_async_remote_copy(
            src_ref=text_all.at[me],
            dst_ref=text_all.at[me],
            send_sem=gather_send,
            recv_sem=gather_recv,
            device_id=peer(k),
            device_id_type=LOGICAL,
        ).start()

    each(1, n, spread)
    pair_in.wait()
    keys_in.wait()
    values_in.wait()

    def all_of(ref, sem):
        some = ref.at[pl.ds(0, n - 1)]
        pltpu.make_async_copy(some, some, sem).wait()

    count = min(CHUNK, n)
    chunks = n // count
    low_one = lax.broadcasted_iota(jnp.int32, (count, LANES), 1) < depth
    rows = lax.broadcasted_iota(jnp.int32, (count, 1), 0)

    def halves(x):
        zero = jnp.zeros_like(x)
        return jnp.concatenate(
            [jnp.where(low_one, x, zero), jnp.where(low_one, zero, x)], axis=0
        ).astype(jnp.bfloat16)

    def joined(x):
        return jnp.where(low_one, x[:count], x[count:])

    def total(terms):
        return jnp.sum(functools.reduce(lambda a, b: a + b, terms), axis=1, keepdims=True)

    def mine_of(base):
        found = jnp.zeros((count, 1), jnp.int32)
        for i in range(count):
            found = jnp.where(rows == i, pairs[base + i], found)
        return jnp.where(found == me, 1.0, -1.0).astype(jnp.float32)

    def tile(ref, j):
        return ref[:, j * LANES : (j + 1) * LANES]

    def one_chunk(base, label, first):
        wide[...] = text_all[pl.ds(base, count)].astype(jnp.float32)
        text = [wide[:, j, :] for j in range(tiles)]
        tnorm = lax.rsqrt(total([t * t for t in text]) / width + EPS)
        normed = [t * tnorm for t in text]
        queries = [halves(t) for t in text]
        every = range(tiles)
        scores = [matmul(queries[j], tile(keys, j), LAST) for j in every]
        tops = [jnp.max(x, axis=1, keepdims=True) for x in scores]
        rate = depth ** (-0.5) * math.log2(math.e)
        raised = [jnp.exp2((x - top) * rate) for x, top in zip(scores, tops)]
        sums = [jnp.sum(x, axis=1, keepdims=True) for x in raised]
        weights = [x * (1.0 / y) for x, y in zip(raised, sums)]
        attn = [x.astype(jnp.bfloat16) for x in weights]
        pooled = [joined(matmul(attn[j], tile(values, j))) for j in every]
        pnorm = lax.rsqrt(total([p * p for p in pooled]) / width + EPS)
        cosine = pnorm * (total([p * t for p, t in zip(pooled, normed)]) / width)
        unit = [p * pnorm for p in pooled]
        logit = LOGIT_SCALE * cosine + LOGIT_BIAS
        z = -label * logit
        loss = jnp.maximum(z, 0.0) + jnp.log1p(jnp.exp(-jnp.abs(z)))
        dcos = LOGIT_SCALE / width * (-label / (1.0 + jnp.exp(-z)))
        into = pnorm * dcos
        back = tnorm * dcos
        dout = [halves(into * (normed[j] - unit[j] * cosine)) for j in every]
        dattn = [matmul(dout[j], tile(values, j), LAST) for j in every]
        levels = [jnp.sum(weights[j] * dattn[j], axis=1, keepdims=True) for j in every]
        dscore = [
            (weights[j] * (dattn[j] - levels[j]) * depth ** (-0.5)).astype(jnp.bfloat16)
            for j in every
        ]
        grads = [joined(matmul(dscore[j], tile(keys, j))) for j in every]
        for j in every:
            part[pl.ds(base, count), j, :] = grads[j] + back * (unit[j] - normed[j] * cosine)
        part[pl.ds(base, count), tiles, :] = jnp.broadcast_to(loss, (count, LANES))

        def deliver(to):
            pltpu.make_async_remote_copy(
                src_ref=part.at[to],
                dst_ref=landed.at[me],
                send_sem=part_send,
                recv_sem=part_recv,
                device_id=to,
                device_id_type=LOGICAL,
            ).start()

        if first:
            each(1, n, lambda k: deliver(peer(k)))
        else:
            each(0, count, lambda k: pl.when(base + k != me)(lambda: deliver(base + k)))
        for j in range(tiles):
            lanes = pl.ds(j, keys.shape[0], stride=tiles)
            gk = matmul(dscore[j], queries[j], FIRST)
            gv = matmul(attn[j], dout[j], FIRST)
            if first:
                keys_out[lanes, :] = gk
                values_out[lanes, :] = gv
            else:
                keys_out[lanes, :] += gk
                values_out[lanes, :] += gv

    if chunks == 1:
        label = mine_of(0)
        all_of(text_all, gather_recv)
        one_chunk(0, label, True)
    else:
        all_of(text_all, gather_recv)
        keys_out[...] = jnp.zeros_like(keys_out)
        values_out[...] = jnp.zeros_like(values_out)

        def body(c, _):
            base = pl.multiple_of(c * count, count)
            one_chunk(base, mine_of(base), False)
            return 0

        lax.fori_loop(0, chunks, body, 0)
    landed[me] = part[me]
    all_of(part, part_recv)
    if chunks == 1:
        got = functools.reduce(lambda a, b: a + b, [landed[i] for i in range(n)])
    else:
        got = lax.fori_loop(
            0, n, lambda i, a: a + landed[i], jnp.zeros(landed.shape[1:], jnp.float32)
        )
    for j in range(tiles):
        text_out[:, j * LANES : (j + 1) * LANES] = got[j : j + 1]
    loss_out[...] = got[tiles : tiles + 1, 0:1] / n
    all_of(text_all, gather_send)
    all_of(part, part_send)


def store(*refs):
    sources, targets, sem = refs[:4], refs[4:8], refs[8]
    copies = [
        pltpu.make_async_copy(source, target, sem.at[i])
        for i, (source, target) in enumerate(zip(sources, targets))
    ]
    for copy in copies:
        copy.start()
    for copy in copies:
        copy.wait()


def local(groups, members, text, keys, values, pair_image):
    n = groups * members
    patches, width = keys.shape[1:]
    tiles = width // LANES
    anywhere = pl.BlockSpec(memory_space=pl.ANY)
    vmem = pl.BlockSpec(memory_space=pltpu.VMEM)
    results = pl.pallas_call(
        functools.partial(kernel, groups, members),
        out_shape=(
            pltpu.VMEM((1, 1), jnp.float32),
            pltpu.VMEM(text.shape, jnp.float32),
            pltpu.VMEM((patches * tiles, LANES), jnp.float32),
            pltpu.VMEM((patches * tiles, LANES), jnp.float32),
        ),
        in_specs=[anywhere] * 4,
        out_specs=(vmem, vmem, vmem, vmem),
        scratch_shapes=[
            pltpu.VMEM(text.shape, jnp.bfloat16),
            pltpu.VMEM((n, tiles, LANES), jnp.bfloat16),
            pltpu.VMEM((min(CHUNK, n), tiles, LANES), jnp.float32),
            pltpu.VMEM((patches, width), jnp.bfloat16),
            pltpu.VMEM((patches, width), jnp.bfloat16),
            pltpu.SMEM((n,), jnp.int32),
            pltpu.VMEM((n, tiles + 1, LANES), jnp.float32),
            pltpu.VMEM((n, tiles + 1, LANES), jnp.float32),
            pltpu.SemaphoreType.DMA((3,)),
            pltpu.SemaphoreType.DMA,
            pltpu.SemaphoreType.DMA,
            pltpu.SemaphoreType.DMA,
            pltpu.SemaphoreType.DMA,
            pltpu.SemaphoreType.DMA,
        ],
        compiler_params=pltpu.CompilerParams(collective_id=0, has_side_effects=True),
        name="pool",
    )(text, keys, values, pair_image)
    results = [pltpu.with_memory_space_constraint(r, pltpu.VMEM) for r in results]
    loss, grad_text, grad_keys, grad_values = pl.pallas_call(
        store,
        out_shape=[jax.ShapeDtypeStruct(r.shape, r.dtype) for r in results],
        in_specs=[vmem] * 4,
        out_specs=[anywhere] * 4,
        scratch_shapes=[pltpu.SemaphoreType.DMA((4,))],
        name="store",
    )(*results)
    return (
        loss.reshape(1),
        grad_text,
        grad_keys.reshape(keys.shape),
        grad_values.reshape(values.shape),
    )


def solution(mesh):
    groups, members = mesh.shape["blk"], mesh.shape["grp"]
    both = ("blk", "grp")
    placed = (P(both, None), P(both, None, None), P(both, None, None), P())
    return jax.shard_map(
        functools.partial(local, groups, members),
        mesh=mesh,
        in_specs=placed,
        out_specs=(P(both), P(both, None), P(both, None, None), P(both, None, None)),
        check_vma=False,
    )
```

```python
import functools
import math

import jax
import jax.numpy as jnp
from jax import lax
from jax.experimental import pallas as pl
from jax.experimental.pallas import tpu as pltpu
from jax.sharding import PartitionSpec as P

HEADS = 8
EPS = 1e-06
LOGIT_SCALE = 10.0
LOGIT_BIAS = -1.0
LANES = 128
CHUNK = 32
LOGICAL = pl.DeviceIdType.LOGICAL
LAST = (((1,), (1,)), ((), ()))
FIRST = (((0,), (0,)), ((), ()))


def matmul(a, b, dims=None):
    if dims is None:
        return jnp.dot(a, b, preferred_element_type=jnp.float32)
    return lax.dot_general(a, b, dims, preferred_element_type=jnp.float32)


def kernel(
    groups, members,
    text_hbm, keys_hbm, values_hbm, pair_hbm,
    loss_out, text_out, keys_out, values_out,
    text_own, text_all, wide, keys, values, pairs, part, landed,
    in_sem, pair_sem, gather_send, gather_recv, part_send, part_recv,
):
    n = groups * members
    width = keys.shape[1]
    tiles = width // LANES
    depth = width // HEADS
    me = lax.axis_index("blk") * members + lax.axis_index("grp")

    def peer(k):
        other = me + k
        return jnp.where(other >= n, other - n, other)

    def each(low, high, step):
        if high - low <= CHUNK:
            for k in range(low, high):
                step(k)
        else:

            def body(k, _):
                step(k)
                return 0

            lax.fori_loop(low, high, body, 0)

    text_in = pltpu.make_async_copy(text_hbm, text_own, in_sem.at[0])
    keys_in = pltpu.make_async_copy(keys_hbm.at[0], keys, in_sem.at[1])
    values_in = pltpu.make_async_copy(values_hbm.at[0], values, in_sem.at[2])
    pair_in = pltpu.make_async_copy(pair_hbm, pairs, pair_sem)
    text_in.start()
    barrier = pltpu.get_barrier_semaphore()

    def greet(k):
        pl.semaphore_signal(barrier, inc=1, device_id=peer(k), device_id_type=LOGICAL)

    each(1, n, greet)
    pair_in.start()
    keys_in.start()
    values_in.start()
    text_in.wait()
    own = text_own[...].astype(jnp.float32)
    text_all[me] = jnp.concatenate(
        [own[:, j * LANES : (j + 1) * LANES] for j in range(tiles)], axis=0
    ).astype(jnp.bfloat16)
    pl.semaphore_wait(barrier, n - 1)

    def spread(to):
        pltpu.make_async_remote_copy(
            src_ref=text_all.at[me],
            dst_ref=text_all.at[me],
            send_sem=gather_send,
            recv_sem=gather_recv,
            device_id=to,
            device_id_type=LOGICAL,
        ).start()

    if n <= CHUNK:
        for to in reversed(range(n)):
            pl.when(to != me)(functools.partial(spread, to))
    else:
        each(1, n, lambda k: spread(peer(k)))
    pair_in.wait()
    keys_in.wait()
    values_in.wait()

    def all_of(ref, sem):
        some = ref.at[pl.ds(0, n - 1)]
        pltpu.make_async_copy(some, some, sem).wait()

    count = min(CHUNK, n)
    chunks = n // count
    low_one = lax.broadcasted_iota(jnp.int32, (count, LANES), 1) < depth
    rows = lax.broadcasted_iota(jnp.int32, (count, 1), 0)

    def halves(x):
        zero = jnp.zeros_like(x)
        return jnp.concatenate(
            [jnp.where(low_one, x, zero), jnp.where(low_one, zero, x)], axis=0
        ).astype(jnp.bfloat16)

    def joined(x):
        return jnp.where(low_one, x[:count], x[count:])

    def total(terms):
        return jnp.sum(functools.reduce(lambda a, b: a + b, terms), axis=1, keepdims=True)

    def mine_of(base):
        found = jnp.zeros((count, 1), jnp.int32)
        for i in range(count):
            found = jnp.where(rows == i, pairs[base + i], found)
        return jnp.where(found == me, 1.0, -1.0).astype(jnp.float32)

    def tile(ref, j):
        return ref[:, j * LANES : (j + 1) * LANES]

    def one_chunk(base, label, first):
        wide[...] = text_all[pl.ds(base, count)].astype(jnp.float32)
        text = [wide[:, j, :] for j in range(tiles)]
        tnorm = lax.rsqrt(total([t * t for t in text]) / width + EPS)
        normed = [t * tnorm for t in text]
        queries = [halves(t) for t in text]
        every = range(tiles)
        scores = [matmul(queries[j], tile(keys, j), LAST) for j in every]
        tops = [jnp.max(x, axis=1, keepdims=True) for x in scores]
        rate = depth ** (-0.5) * math.log2(math.e)
        raised = [jnp.exp2((x - top) * rate) for x, top in zip(scores, tops)]
        sums = [jnp.sum(x, axis=1, keepdims=True) for x in raised]
        weights = [x * (1.0 / y) for x, y in zip(raised, sums)]
        attn = [x.astype(jnp.bfloat16) for x in weights]
        pooled = [joined(matmul(attn[j], tile(values, j))) for j in every]
        pnorm = lax.rsqrt(total([p * p for p in pooled]) / width + EPS)
        cosine = pnorm * (total([p * t for p, t in zip(pooled, normed)]) / width)
        unit = [p * pnorm for p in pooled]
        logit = LOGIT_SCALE * cosine + LOGIT_BIAS
        z = -label * logit
        loss = jnp.maximum(z, 0.0) + jnp.log1p(jnp.exp(-jnp.abs(z)))
        dcos = LOGIT_SCALE / width * (-label / (1.0 + jnp.exp(-z)))
        into = pnorm * dcos
        back = tnorm * dcos
        dout = [halves(into * (normed[j] - unit[j] * cosine)) for j in every]
        dattn = [matmul(dout[j], tile(values, j), LAST) for j in every]
        levels = [jnp.sum(weights[j] * dattn[j], axis=1, keepdims=True) for j in every]
        dscore = [
            (weights[j] * (dattn[j] - levels[j]) * depth ** (-0.5)).astype(jnp.bfloat16)
            for j in every
        ]
        grads = [joined(matmul(dscore[j], tile(keys, j))) for j in every]
        for j in every:
            part[pl.ds(base, count), j, :] = grads[j] + back * (unit[j] - normed[j] * cosine)
        part[pl.ds(base, count), tiles, :] = jnp.broadcast_to(loss, (count, LANES))

        def deliver(to):
            pltpu.make_async_remote_copy(
                src_ref=part.at[to],
                dst_ref=landed.at[me],
                send_sem=part_send,
                recv_sem=part_recv,
                device_id=to,
                device_id_type=LOGICAL,
            ).start()

        if first:
            each(1, n, lambda k: deliver(peer(k)))
        else:
            each(0, count, lambda k: pl.when(base + k != me)(lambda: deliver(base + k)))
        for j in range(tiles):
            lanes = pl.ds(j, keys.shape[0], stride=tiles)
            gk = matmul(dscore[j], queries[j], FIRST)
            gv = matmul(attn[j], dout[j], FIRST)
            if first:
                keys_out[lanes, :] = gk
                values_out[lanes, :] = gv
            else:
                keys_out[lanes, :] += gk
                values_out[lanes, :] += gv

    if chunks == 1:
        label = mine_of(0)
        all_of(text_all, gather_recv)
        one_chunk(0, label, True)
    else:
        all_of(text_all, gather_recv)
        keys_out[...] = jnp.zeros_like(keys_out)
        values_out[...] = jnp.zeros_like(values_out)

        def body(c, _):
            base = pl.multiple_of(c * count, count)
            one_chunk(base, mine_of(base), False)
            return 0

        lax.fori_loop(0, chunks, body, 0)
    landed[me] = part[me]
    all_of(part, part_recv)
    if chunks == 1:
        got = functools.reduce(lambda a, b: a + b, [landed[i] for i in range(n)])
    else:
        got = lax.fori_loop(
            0, n, lambda i, a: a + landed[i], jnp.zeros(landed.shape[1:], jnp.float32)
        )
    for j in range(tiles):
        text_out[:, j * LANES : (j + 1) * LANES] = got[j : j + 1]
    loss_out[...] = got[tiles : tiles + 1, 0:1] / n
    all_of(text_all, gather_send)
    all_of(part, part_send)


def store(*refs):
    sources, targets, sem = refs[:4], refs[4:8], refs[8]
    copies = [
        pltpu.make_async_copy(source, target, sem.at[i])
        for i, (source, target) in enumerate(zip(sources, targets))
    ]
    for copy in copies:
        copy.start()
    for copy in copies:
        copy.wait()


def local(groups, members, text, keys, values, pair_image):
    n = groups * members
    patches, width = keys.shape[1:]
    tiles = width // LANES
    anywhere = pl.BlockSpec(memory_space=pl.ANY)
    vmem = pl.BlockSpec(memory_space=pltpu.VMEM)
    results = pl.pallas_call(
        functools.partial(kernel, groups, members),
        out_shape=(
            pltpu.VMEM((1, 1), jnp.float32),
            pltpu.VMEM(text.shape, jnp.float32),
            pltpu.VMEM((patches * tiles, LANES), jnp.float32),
            pltpu.VMEM((patches * tiles, LANES), jnp.float32),
        ),
        in_specs=[anywhere] * 4,
        out_specs=(vmem, vmem, vmem, vmem),
        scratch_shapes=[
            pltpu.VMEM(text.shape, jnp.bfloat16),
            pltpu.VMEM((n, tiles, LANES), jnp.bfloat16),
            pltpu.VMEM((min(CHUNK, n), tiles, LANES), jnp.float32),
            pltpu.VMEM((patches, width), jnp.bfloat16),
            pltpu.VMEM((patches, width), jnp.bfloat16),
            pltpu.SMEM((n,), jnp.int32),
            pltpu.VMEM((n, tiles + 1, LANES), jnp.float32),
            pltpu.VMEM((n, tiles + 1, LANES), jnp.float32),
            pltpu.SemaphoreType.DMA((3,)),
            pltpu.SemaphoreType.DMA,
            pltpu.SemaphoreType.DMA,
            pltpu.SemaphoreType.DMA,
            pltpu.SemaphoreType.DMA,
            pltpu.SemaphoreType.DMA,
        ],
        compiler_params=pltpu.CompilerParams(collective_id=0, has_side_effects=True),
        name="pool",
    )(text, keys, values, pair_image)
    results = [pltpu.with_memory_space_constraint(r, pltpu.VMEM) for r in results]
    loss, grad_text, grad_keys, grad_values = pl.pallas_call(
        store,
        out_shape=[jax.ShapeDtypeStruct(r.shape, r.dtype) for r in results],
        in_specs=[vmem] * 4,
        out_specs=[anywhere] * 4,
        scratch_shapes=[pltpu.SemaphoreType.DMA((4,))],
        name="store",
    )(*results)
    return (
        loss.reshape(1),
        grad_text,
        grad_keys.reshape(keys.shape),
        grad_values.reshape(values.shape),
    )


def solution(mesh):
    groups, members = mesh.shape["blk"], mesh.shape["grp"]
    both = ("blk", "grp")
    placed = (P(both, None), P(both, None, None), P(both, None, None), P())
    return jax.shard_map(
        functools.partial(local, groups, members),
        mesh=mesh,
        in_specs=placed,
        out_specs=(P(both), P(both, None), P(both, None, None), P(both, None, None)),
        check_vma=False,
    )
```
